256 devices in a mesh: grp: 2 (over z), freq: 64 (over x, y), pair: 2 (over core).
Axes of the slice: x: 8, y: 8, z: 2, core: 2. Of those that a mesh axis runs over, the one named last changes fastest.
The devices are a block of a 8x8x16 slice.
Arguments:
- spectra: bfloat16 [384, 1024, 2, 512], P(('grp', 'pair'), 'freq'), parts along dimension 0, may hold values from -6 to 6
- valid: int32 [384, 512], P(('grp', 'pair')), parts along dimension 0, may hold values 0 or 1
- ref_spectra: bfloat16 [384, 1024, 2, 256], P(('grp', 'pair'), 'freq'), parts along dimension 0, may hold values from -6 to 6
- ref_valid: int32 [384, 256], P(('grp', 'pair')), parts along dimension 0, may hold values 0 or 1
Outputs:
- xcorr: float32 [802, 512, 256], P('grp', ('freq', 'pair')), parts along dimension 0
The draws below stay inside these ranges and needn't reach their ends.
There are 2 independent parts, one for each index of `grp`. The reference program is written for one: setup_inputs(seed, part) draws one part's arguments, and reference() takes and returns one part's arrays. A program takes and returns all parts, laid end to end along the dimension named above; each array names one. Nothing has to cross between parts.
All inputs are finite; a program needn't handle non-finite values. No bound on the sum of `valid` or of `ref_valid` on one device may be relied on, other than what follows from the above.
Results may differ from the reference program's by a relative error of at most 0.0054.
Values may be sent and summed in bfloat16 or wider, within the bound.
No kernel may reach another device: no remote copies, remote signals or barrier semaphores. Data moves between devices by JAX's collectives and lax.ppermute only.
A program may use at most 192 MiB of HBM per device.

```python
import jax
import jax.numpy as jnp
from jax import lax

S = 512
F = 1024
LAGS = 401
REACH = 10
SRC = 256
W = 192


def plant(drawn, rng, least, top_value):
    index_at = [jax.random.randint(jax.random.fold_in(rng, axis), (), 0, length) for axis, length in enumerate(drawn.shape)]
    widest = drawn.shape.index(max(drawn.shape))
    beside = index_at[:widest] + [(index_at[widest] + 1) % drawn.shape[widest]] + index_at[widest + 1:]
    return drawn.at[tuple(index_at)].set(least).at[tuple(beside)].set(top_value)


def shard_levels(rng, shape, cuts, low, top_value):
    def one(axis_at, parts):
        heights = jax.random.uniform(jax.random.fold_in(jax.random.fold_in(rng, 6), axis_at), (parts,), jnp.float32, low / len(cuts), top_value / len(cuts))
        return jnp.repeat(jnp.exp(heights), shape[axis_at] // parts).reshape((-1,) + (1,) * (len(shape) - axis_at - 1))

    gain = one(*cuts[0])
    for cut in cuts[1:]:
        gain = gain * one(*cut)
    return gain


def scatter_about(key, extent, deviation, reach, pieces=(), kind=jnp.bfloat16):
    drawn = jax.random.normal(key, extent, jnp.float32) * deviation
    if len(pieces) > 0:
        drawn = shard_levels(key, extent, pieces, -0.22, 0.18) * drawn
    return jnp.clip(drawn, min=-reach, max=reach).astype(kind)


def setup_inputs(seed: int = 0, part: int = 0) -> dict:
    seeds = jax.random.split(jax.random.key(seed), 5)
    part_splits = jax.random.split(jax.random.fold_in(seeds[4], part), 5)
    return {
        "spectra": scatter_about(part_splits[0], (W, F, 2, S), 1.0, 6.0, ((0, 2), (1, 64))),
        "valid": plant((jax.random.randint(part_splits[1], (W, S), 0, 4) < 3).astype(jnp.int32), jax.random.fold_in(part_splits[1], 1), 0, 1),
        "ref_spectra": scatter_about(part_splits[2], (W, F, 2, SRC), 1.0, 6.0, ((0, 2), (1, 64))),
        "ref_valid": plant((jax.random.randint(part_splits[3], (W, SRC), 0, 4) < 3).astype(jnp.int32), jax.random.fold_in(part_splits[3], 1), 0, 1),
    }


water_level = 0.1
block_bins = 64

def power_of(spectra):
    real_part = spectra[:, :, 0].astype(jnp.float32)
    imag_part = spectra[:, :, 1].astype(jnp.float32)
    return real_part * real_part + imag_part * imag_part

def lag_table(first_bin, bin_total):
    bin_index = first_bin + jnp.arange(bin_total, dtype=jnp.int32)
    offsets = jnp.arange(LAGS, dtype=jnp.int32) - (LAGS - 1) // 2
    phases = jnp.mod(offsets[:, None] * bin_index[None, :], F).astype(jnp.float32) * (2.0 * jnp.pi / F)
    norm_scale = 1.0 / jnp.sqrt(jnp.float32(F))
    return jnp.stack([jnp.cos(phases) * norm_scale, -jnp.sin(phases) * norm_scale], axis=1).astype(jnp.bfloat16)

def rotated(white):
    turned = jnp.stack([-white[:, :, 1], white[:, :, 0]], axis=2)
    return jnp.concatenate([white, turned], axis=3)

def whiten(spectra, validity, padded, first_bin):
    window = lax.dynamic_slice_in_dim(padded, first_bin, block_bins + 2 * REACH, 1)
    smooth = window[:, 0:block_bins]
    for offset_bins in range(1, 2 * REACH + 1):
        smooth = smooth + window[:, offset_bins:offset_bins + block_bins]
    smooth = smooth / (2 * REACH + 1)
    spectrum = lax.dynamic_slice_in_dim(spectra, first_bin, block_bins, 1).astype(jnp.float32)
    inverse_amp = lax.rsqrt(smooth + water_level) * validity.astype(jnp.float32)[:, None, :]
    return (spectrum * inverse_amp[:, :, None, :]).astype(jnp.bfloat16)

def reference(spectra, valid, ref_spectra, ref_valid):
    stations = spectra.shape[3]
    sources = ref_spectra.shape[3]
    padding = ((0, 0), (REACH, REACH), (0, 0))
    rec_padded = jnp.pad(power_of(spectra), padding)
    ref_padded = jnp.pad(power_of(ref_spectra), padding)
    pair_count = jnp.dot(valid.astype(jnp.float32).T, ref_valid.astype(jnp.float32), precision=lax.Precision.HIGHEST)
    norm_factor = jnp.sqrt(pair_count + 1.0)

    def accumulate(summed, block_index):
        first_bin = (block_index * block_bins).astype(jnp.int32)
        rec_white = whiten(spectra, valid, rec_padded, first_bin)
        ref_white = whiten(ref_spectra, ref_valid, ref_padded, first_bin)
        ref_both = rotated(ref_white)
        cross_gram = jnp.einsum('wfcj,wfck->fjk', rec_white.astype(jnp.float32), ref_both.astype(jnp.float32), precision=lax.Precision.HIGHEST)
        stacked = (cross_gram.reshape(block_bins, stations, 2, sources) / norm_factor[None, :, None, :]).astype(jnp.bfloat16)
        lag_weights = lag_table(first_bin, block_bins)
        summed = summed + jnp.einsum('fjcs,lcf->ljs', stacked.astype(jnp.float32), lag_weights.astype(jnp.float32), precision=lax.Precision.HIGHEST)
        return (summed, None)
    summed = jnp.zeros((LAGS, stations, sources), jnp.float32)
    summed, unused = lax.scan(accumulate, summed, jnp.arange(F // block_bins, dtype=jnp.int32))
    return summed
```

```python
import functools

import jax
import jax.numpy as jnp
from jax import lax
from jax.experimental import pallas as pl
from jax.experimental.pallas import tpu as pltpu
from jax.sharding import PartitionSpec as P

LAGS = 401
REACH = 10
LANES = 128
WATER_LEVEL = 0.1


def cost(flops, transferred, transcendentals=0):
    return pl.CostEstimate(
        flops=int(flops), bytes_accessed=int(transferred), transcendentals=int(transcendentals)
    )


def power_of(spectra):
    real_part = spectra[:, 0].astype(jnp.float32)
    imag_part = spectra[:, 1].astype(jnp.float32)
    return real_part * real_part + imag_part * imag_part


def neighbour_powers(spectra, ref_spectra):
    count = lax.axis_size("freq")
    up = [(i, i + 1) for i in range(count - 1)]
    down = [(j, i) for i, j in up]
    bins = spectra.shape[0]

    def edge(first, last):
        return jnp.concatenate(
            [power_of(spectra[first:last]), power_of(ref_spectra[first:last])], axis=2
        ).astype(jnp.bfloat16)

    before = lax.ppermute(edge(bins - REACH, bins), "freq", up)
    after = lax.ppermute(edge(0, REACH), "freq", down)
    return before, after


def smoothed(own, before, after):
    row = before + own + after
    bins = len(own)
    first, last = bins - 1, 2 * REACH + 1
    middle = functools.reduce(jnp.add, row[first:last])
    left = [None] * bins
    for f in range(bins - 2, -1, -1):
        left[f] = row[f] if left[f + 1] is None else left[f + 1] + row[f]
    right = [None] * bins
    for f in range(1, bins):
        end = row[f + 2 * REACH]
        right[f] = end if right[f - 1] is None else right[f - 1] + end
    means = []
    for f in range(bins):
        total = middle
        if left[f] is not None:
            total = total + left[f]
        if right[f] is not None:
            total = total + right[f]
        means.append(total * (1.0 / (2 * REACH + 1)))
    return means


def whiten_kernel(
    rec_ref, src_ref, before_ref, after_ref, valid_ref, src_valid_ref, order_ref,
    keep_ref, send_ref, white_ref,
):
    bins, _, rows, stations = rec_ref.shape
    sources = src_ref.shape[3]
    half = stations // 2

    def tile(spectra_ref, valid, at, lane, put):
        lanes = pl.ds(lane, LANES)
        sides = pl.ds(at + lane, LANES)
        parts = [
            [spectra_ref[f, c, :, lanes].astype(jnp.float32) for c in range(2)]
            for f in range(bins)
        ]
        means = smoothed(
            [re * re + im * im for re, im in parts],
            [before_ref[k, :, sides].astype(jnp.float32) for k in range(REACH)],
            [after_ref[k, :, sides].astype(jnp.float32) for k in range(REACH)],
        )
        weight = valid[:, lanes].astype(jnp.float32)
        for f in range(bins):
            gain = lax.rsqrt(means[f] + WATER_LEVEL) * weight
            for c in range(2):
                put(2 * f + c, lanes, (parts[f][c] * gain).astype(jnp.bfloat16))

    def put_rec(row, lanes, value):
        white_ref[row, :, lanes] = value

    def put_src(row, lanes, value):
        send_ref[2 * bins + row, :, lanes] = value

    for lane in range(0, stations, LANES):
        tile(rec_ref, valid_ref, 0, lane, put_rec)
    for lane in range(0, sources, LANES):
        tile(src_ref, src_valid_ref, stations, lane, put_src)
    order = order_ref[...]
    ordered = jnp.dot(
        white_ref[...].reshape(2 * bins * rows, stations), order, preferred_element_type=jnp.float32
    ).astype(jnp.bfloat16)
    keep_ref[0 : 2 * bins] = ordered[:, :half].reshape(2 * bins, rows, half)
    send_ref[0 : 2 * bins] = ordered[:, half:].reshape(2 * bins, rows, half)
    valid = jnp.dot(
        valid_ref[...].astype(jnp.float32).astype(jnp.bfloat16),
        order,
        preferred_element_type=jnp.float32,
    ).astype(jnp.bfloat16)
    keep_ref[2 * bins] = valid[:, :half]
    send_ref[4 * bins] = valid[:, half:]
    send_ref[4 * bins + 1] = src_valid_ref[...].astype(jnp.float32).astype(jnp.bfloat16)


def whitened(spectra, ref_spectra, before, after, valid, ref_valid, order):
    bins, _, windows, stations = spectra.shape
    sources = ref_spectra.shape[3]
    half = stations // 2
    assert half == sources
    rows = 16
    return pl.pallas_call(
        whiten_kernel,
        grid=(windows // rows,),
        in_specs=[
            pl.BlockSpec((bins, 2, rows, stations), lambda w: (0, 0, w, 0)),
            pl.BlockSpec((bins, 2, rows, sources), lambda w: (0, 0, w, 0)),
            pl.BlockSpec((REACH, rows, stations + sources), lambda w: (0, w, 0)),
            pl.BlockSpec((REACH, rows, stations + sources), lambda w: (0, w, 0)),
            pl.BlockSpec((rows, stations), lambda w: (w, 0)),
            pl.BlockSpec((rows, sources), lambda w: (w, 0)),
            pl.BlockSpec((stations, stations), lambda w: (0, 0)),
        ],
        out_specs=[
            pl.BlockSpec((2 * bins + 1, rows, half), lambda w: (0, w, 0)),
            pl.BlockSpec((4 * bins + 2, rows, half), lambda w: (0, w, 0)),
        ],
        out_shape=[
            jax.ShapeDtypeStruct((2 * bins + 1, windows, half), jnp.bfloat16),
            jax.ShapeDtypeStruct((4 * bins + 2, windows, half), jnp.bfloat16),
        ],
        scratch_shapes=[pltpu.VMEM((2 * bins, rows, stations), jnp.bfloat16)],
        compiler_params=pltpu.CompilerParams(vmem_limit_bytes=40 << 20),
        cost_estimate=cost(2 * windows * 2 * bins * stations * stations, 14 << 20),
        name="whiten",
    )(spectra, ref_spectra, before, after, valid, ref_valid, order)


def over_windows(left, right):
    return lax.dot_general(
        left, right, (((0,), (0,)), ((), ())), preferred_element_type=jnp.float32
    )


def stack_kernel(
    own_rec, own_src, their_rec, their_src, own_valid, own_src_valid, their_valid, their_src_valid,
    out_ref, norm_ref, wide_ref,
):
    f = pl.program_id(0)
    blocks, depth, width = out_ref.shape
    columns = own_src.shape[2]
    parts = width // columns

    @pl.when(f == 0)
    def _():
        count = over_windows(own_valid[0], own_src_valid[0])
        count = count + over_windows(their_valid[0], their_src_valid[0])
        norm_ref[...] = lax.rsqrt(count + 1.0)

    row = lax.rem(f, depth // 2) * 2
    norm = norm_ref[...]

    def gram(turned):
        total = None
        for rec, src in ((own_rec, own_src), (their_rec, their_src)):
            windows = rec.shape[1]
            left = rec[...].reshape(2 * windows, columns)
            if turned:
                right = jnp.concatenate([-src[1], src[0]], axis=0)
            else:
                right = src[...].reshape(2 * windows, columns)
            part = over_windows(left, right)
            total = part if total is None else total + part
        return total * norm

    for c in range(2):
        value = gram(c == 1)
        for r in range(parts):
            for lane in range(0, columns, LANES):
                tile = (r * columns + lane) // LANES
                wide_ref[tile, pl.ds(row + c, blocks, stride=depth), :] = value[
                    r * blocks : (r + 1) * blocks, lane : lane + LANES
                ]

    @pl.when(row == depth - 2)
    def _():
        for tile in range(width // LANES):
            out_ref[:, :, tile * LANES : (tile + 1) * LANES] = (
                wide_ref[tile].reshape(blocks, depth, LANES).astype(jnp.bfloat16)
            )


def stacked_blocks(keep, send, received, blocks):
    rows, windows, half = send.shape
    bins = (rows - 2) // 4
    parts = half // blocks
    depth = 16

    def two(at):
        return pl.BlockSpec((2, windows, half), lambda f: (at + f, 0, 0))

    def one(at):
        return pl.BlockSpec((1, windows, half), lambda f: (at, 0, 0))

    return pl.pallas_call(
        stack_kernel,
        grid=(bins,),
        in_specs=[
            two(0), two(bins), two(0), two(bins),
            one(2 * bins), one(4 * bins + 1), one(4 * bins), one(4 * bins + 1),
        ],
        out_specs=pl.BlockSpec(
            (blocks, depth, parts * half), lambda f: (0, lax.div(2 * f, depth), 0)
        ),
        out_shape=jax.ShapeDtypeStruct((blocks, 2 * bins, parts * half), jnp.bfloat16),
        scratch_shapes=[
            pltpu.VMEM((half, half), jnp.float32),
            pltpu.VMEM((parts * half // LANES, blocks * depth, LANES), jnp.float32),
        ],
        compiler_params=pltpu.CompilerParams(vmem_limit_bytes=40 << 20),
        cost_estimate=cost(8 * bins * windows * 2 * half * half, 12 << 20),
        name="stack",
    )(keep, send, received, received, keep, send, received, received)


def lag_kernel(weights_ref, blocks_ref, out_ref):
    parts, columns = out_ref.shape[1:]
    total = jnp.dot(weights_ref[...], blocks_ref[...], preferred_element_type=jnp.float32)
    for r in range(parts):
        out_ref[:, r, :] = total[:, r * columns : (r + 1) * columns]


def to_lags(weights, blocks, parts):
    depth, width = blocks.shape
    rows = 104
    return pl.pallas_call(
        lag_kernel,
        grid=(weights.shape[0] // rows,),
        in_specs=[
            pl.BlockSpec((rows, depth), lambda l: (l, 0)),
            pl.BlockSpec((depth, width), lambda l: (0, 0)),
        ],
        out_specs=pl.BlockSpec((rows, parts, width // parts), lambda l: (l, 0, 0)),
        out_shape=jax.ShapeDtypeStruct((LAGS, parts, width // parts), jnp.float32),
        compiler_params=pltpu.CompilerParams(vmem_limit_bytes=40 << 20),
        cost_estimate=cost(2 * weights.shape[0] * depth * width, 8 << 20),
        name="lags",
    )(weights, blocks)


def lag_table(bin_total, rows):
    column = jnp.arange(2 * bin_total, dtype=jnp.int32)
    offset = jnp.arange(rows, dtype=jnp.int32) - (LAGS - 1) // 2
    turns = offset[:, None] * (column // 2)[None, :] + (column % 2)[None, :] * (bin_total // 4)
    phases = jnp.mod(turns, bin_total).astype(jnp.float32) * (2.0 * jnp.pi / bin_total)
    return (jnp.cos(phases) * (1.0 / jnp.sqrt(jnp.float32(bin_total)))).astype(jnp.bfloat16)


def station_order(stations, blocks, pairs):
    column = jnp.arange(stations, dtype=jnp.int32)
    share = stations // pairs
    each = share // blocks
    owner = column % blocks
    receiver = (column // blocks) % each
    pair = (column // share + lax.axis_index("pair")) % pairs
    source = (owner * pairs + pair) * each + receiver
    return (jnp.arange(stations, dtype=jnp.int32)[:, None] == source[None, :]).astype(jnp.bfloat16)


def local(spectra, valid, ref_spectra, ref_valid):
    stations = spectra.shape[3]
    freq_devs = lax.axis_size("freq")
    pair_devs = lax.axis_size("pair")
    bin_total = spectra.shape[1] * freq_devs
    parts = stations // (freq_devs * pair_devs)
    rec = jnp.transpose(spectra, (1, 2, 0, 3))
    src = jnp.transpose(ref_spectra, (1, 2, 0, 3))
    before, after = neighbour_powers(rec, src)
    order = station_order(stations, freq_devs, pair_devs)
    weights = lag_table(bin_total, 416)
    keep, send = whitened(rec, src, before, after, valid, ref_valid, order)
    swap = [(i, (i + 1) % pair_devs) for i in range(pair_devs)]
    received = lax.ppermute(send, "pair", swap)
    blocks = stacked_blocks(keep, send, received, freq_devs)
    arrived = lax.all_to_all(blocks, "freq", 0, 0, tiled=True)
    return to_lags(weights, arrived.reshape(2 * bin_total, -1), parts)


def solution(mesh):
    placed = (
        P(("grp", "pair"), "freq", None, None),
        P(("grp", "pair"), None),
        P(("grp", "pair"), "freq", None, None),
        P(("grp", "pair"), None),
    )
    return jax.shard_map(
        local,
        mesh=mesh,
        in_specs=placed,
        out_specs=P("grp", ("freq", "pair"), None),
        check_vma=False,
    )
```
